16 devices in a mesh: tp: 2 (over z), dp: 2 (over y), pp: 4 (over x, core).
Axes of the slice: x: 2, y: 2, z: 2, core: 2. Of those that a mesh axis runs over, the one named last changes fastest.
Arguments:
- master: float32 [32000, 1152], P('tp')
- exp_avg: float32 [32000, 1152], P('tp')
- exp_avg_sq: float32 [32000, 1152], P('tp')
- stage_ids: int32 [4, 12, 768], P('pp', 'dp')
- stage_acts: bfloat16 [4, 12, 768, 1152], P('pp', 'dp')
Outputs:
- output 1: float32 [32000, 1152], P('tp')
- output 2: float32 [32000, 1152], P('tp')
- output 3: float32 [32000, 1152], P('tp')
- output 4: bfloat16 [32000, 1152], P('tp')
All inputs are finite; a program needn't handle non-finite values.
Results may differ from the reference program's by a relative error of at most 0.001.
Values sent between devices are 32-bit elements.
A program may use at most 2 GiB of HBM per device.

```python
import math
import jax
import jax.numpy as jnp
from jax import lax

VOCAB_SIZE = 32000
MODEL_DIM = 1152
SEQ_LEN = 768
BATCH_DEV = 6
DATA_REPL = 2
PIPE_STAGES = 4
OPT_STEP = 10
TOKEN_BLOCK = 128

BATCH_ALL = BATCH_DEV * DATA_REPL
TOKENS_REPL = BATCH_DEV * SEQ_LEN
LOG_SPAN = math.ceil(math.log2(VOCAB_SIZE))
LEARN_RATE = 0.003
BETA_ONE = 0.9
BETA_TWO = 0.95
ADAM_EPS = 1e-8
WEIGHT_DECAY = 0.1
CLIP_NORM = 1.0


def draw_ids(key, perm):
    key_exp, key_rank = jax.random.split(key)
    ids_shape = (PIPE_STAGES, BATCH_ALL, SEQ_LEN)
    exponents = jax.random.randint(key_exp, ids_shape, 0, LOG_SPAN + 1)
    upper_bound = jnp.minimum(jnp.left_shift(jnp.int32(1), exponents), VOCAB_SIZE)
    ranks = jax.random.randint(key_rank, ids_shape, 0, upper_bound)
    tokens = perm[ranks]
    tokens = tokens.at[:, 0, 0].set(0)
    tokens = tokens.at[:, BATCH_ALL - 1, SEQ_LEN - 1].set(VOCAB_SIZE - 1)
    return tokens.astype(jnp.int32)


def setup_inputs(seed: int = 0) -> dict:
    key = jax.random.key(seed)
    k_tab, k_avg, k_sq, k_perm, k_ids, k_act, k_hid = jax.random.split(key, 7)
    table_shape = (VOCAB_SIZE, MODEL_DIM)
    elem_scale = (VOCAB_SIZE * MODEL_DIM) ** -0.5
    master = jax.random.normal(k_tab, table_shape, jnp.float32) * MODEL_DIM ** -0.5
    exp_avg = jax.random.normal(k_avg, table_shape, jnp.float32) * (0.3 * elem_scale)
    exp_avg_sq = jnp.exp(0.5 * jax.random.normal(k_sq, table_shape, jnp.float32)) * (0.09 * elem_scale * elem_scale)
    perm = jax.random.permutation(k_perm, VOCAB_SIZE)
    stage_ids = draw_ids(k_ids, perm)
    grad_scale = 0.08 * math.sqrt(DATA_REPL / TOKENS_REPL)
    stage_acts = jax.random.normal(k_act, (PIPE_STAGES, BATCH_ALL, SEQ_LEN, MODEL_DIM), jnp.float32) * grad_scale
    label_pull = math.log(VOCAB_SIZE) / math.sqrt(MODEL_DIM)
    noise = jax.random.normal(k_hid, (BATCH_ALL, SEQ_LEN, MODEL_DIM), jnp.float32)
    hidden = math.sqrt(1.0 - label_pull * label_pull) * noise + (label_pull * math.sqrt(MODEL_DIM)) * master[stage_ids[PIPE_STAGES - 1]]
    stage_acts = stage_acts.at[PIPE_STAGES - 1].set(hidden)
    return {"master": master, "exp_avg": exp_avg, "exp_avg_sq": exp_avg_sq, "stage_ids": stage_ids, "stage_acts": stage_acts.astype(jnp.bfloat16)}


def head_block(table_bf, hid_block, lab_block):
    logits = jnp.dot(hid_block, table_bf.T, preferred_element_type=jnp.float32)
    prob_mat = jax.nn.softmax(logits, axis=-1)
    is_label = lab_block[:, None] == jnp.arange(VOCAB_SIZE, dtype=jnp.int32)[None, :]
    dlogits = (jnp.where(is_label, prob_mat - 1.0, prob_mat) / TOKENS_REPL).astype(jnp.bfloat16)
    return jnp.dot(dlogits.T, hid_block, preferred_element_type=jnp.float32)


def replica_grad(table_bf, ids_in, dx_in, hidden, labels):
    grad_embed = jax.ops.segment_sum(dx_in.astype(jnp.float32), ids_in, num_segments=VOCAB_SIZE)

    def add_block(acc_grad, block_in):
        return acc_grad + head_block(table_bf, block_in[0], block_in[1]), None

    hid_blocks = hidden.reshape(-1, TOKEN_BLOCK, MODEL_DIM)
    lab_blocks = labels.reshape(-1, TOKEN_BLOCK)
    return lax.scan(add_block, grad_embed, (hid_blocks, lab_blocks))[0]


def reference(master, exp_avg, exp_avg_sq, stage_ids, stage_acts):
    table_bf = master.astype(jnp.bfloat16)
    ids_in = stage_ids[0].reshape(DATA_REPL, TOKENS_REPL)
    labels = stage_ids[PIPE_STAGES - 1].reshape(DATA_REPL, TOKENS_REPL)
    dx_in = stage_acts[0].reshape(DATA_REPL, TOKENS_REPL, MODEL_DIM)
    hidden = stage_acts[PIPE_STAGES - 1].reshape(DATA_REPL, TOKENS_REPL, MODEL_DIM)

    def add_replica(acc_grad, block_in):
        return acc_grad + replica_grad(table_bf, block_in[0], block_in[1], block_in[2], block_in[3]), None

    zero_grad = jnp.zeros((VOCAB_SIZE, MODEL_DIM), jnp.float32)
    grad_sum = lax.scan(add_replica, zero_grad, (ids_in, dx_in, hidden, labels))[0]
    gradient = grad_sum / DATA_REPL
    norm_val = jnp.sqrt(jnp.sum(gradient * gradient))
    gradient = gradient * (CLIP_NORM / jnp.maximum(norm_val, CLIP_NORM))
    new_avg = BETA_ONE * exp_avg + (1.0 - BETA_ONE) * gradient
    new_avg_sq = BETA_TWO * exp_avg_sq + (1.0 - BETA_TWO) * gradient * gradient
    corr_one = 1.0 - BETA_ONE ** OPT_STEP
    corr_two = 1.0 - BETA_TWO ** OPT_STEP
    step_dir = (new_avg / corr_one) / (jnp.sqrt(new_avg_sq / corr_two) + ADAM_EPS)
    new_master = master - LEARN_RATE * (step_dir + WEIGHT_DECAY * master)
    return new_master, new_avg, new_avg_sq, new_master.astype(jnp.bfloat16)
```

```python
import functools

import jax
import jax.numpy as jnp
from jax import lax
from jax.experimental import pallas as pl
from jax.experimental.pallas import tpu as pltpu
from jax.sharding import PartitionSpec as P

LEARN_RATE = 0.003
BETA_ONE = 0.9
BETA_TWO = 0.95
ADAM_EPS = 1e-8
WEIGHT_DECAY = 0.1
CLIP_NORM = 1.0
OPT_STEP = 10

ROW_TILE = 800
LOOK_TILE = 400
LOOK_CHUNK = 256
ADAM_TILE = 200
VMEM_LIMIT = 63 * 1024 * 1024
LOWEST = float(jnp.finfo(jnp.float32).min)


def params(n_axes):
    return pltpu.CompilerParams(dimension_semantics=("arbitrary",) * n_axes, vmem_limit_bytes=VMEM_LIMIT)


def logits_kernel(idx_ref, hid_ref, tab_ref, *refs):
    out_ref, hid_out, max_out, sum_out, max_scr, sum_scr = refs[-6:]
    step = pl.program_id(0)

    @pl.when(step == 0)
    def _():
        hid_out[...] = hid_ref[...].astype(jnp.bfloat16)
        max_scr[...] = jnp.full_like(max_scr, LOWEST)
        sum_scr[...] = jnp.zeros_like(sum_scr)

    logits = lax.dot_general(tab_ref[...], hid_out[...], (((1,), (1,)), ((), ())), preferred_element_type=jnp.float32)
    out_ref[...] = logits
    rows, toks = logits.shape
    grouped = logits.reshape(rows // 8, 8, toks)
    old_max = max_scr[...]
    new_max = jnp.maximum(old_max, jnp.max(grouped, axis=0))
    sum_scr[...] = sum_scr[...] * jnp.exp(old_max - new_max) + jnp.sum(jnp.exp(grouped - new_max[None]), axis=0)
    max_scr[...] = new_max

    @pl.when(step == pl.num_programs(0) - 1)
    def _():
        top = jnp.max(max_scr[...], axis=0, keepdims=True)
        max_out[...] = top[None]
        sum_out[...] = jnp.sum(sum_scr[...] * jnp.exp(max_scr[...] - top), axis=0, keepdims=True)[None]


def logits_call(idx, hid, tab, bufs, n_chunk):
    rows, dim = tab.shape
    toks = hid.shape[0]
    shapes = [
        jax.ShapeDtypeStruct((rows, n_chunk * toks), jnp.float32),
        jax.ShapeDtypeStruct((n_chunk * toks, dim), jnp.bfloat16),
        jax.ShapeDtypeStruct((n_chunk, 1, toks), jnp.float32),
        jax.ShapeDtypeStruct((n_chunk, 1, toks), jnp.float32),
    ]
    extra = list(bufs) if bufs is not None else []
    return pl.pallas_call(
        logits_kernel,
        out_shape=shapes,
        grid_spec=pltpu.PrefetchScalarGridSpec(
            num_scalar_prefetch=1,
            grid=(rows // ROW_TILE,),
            in_specs=[
                pl.BlockSpec((toks, dim), lambda i, s: (0, 0)),
                pl.BlockSpec((ROW_TILE, dim), lambda i, s: (i, 0)),
            ] + [pl.BlockSpec(memory_space=pl.ANY)] * len(extra),
            out_specs=[
                pl.BlockSpec((ROW_TILE, toks), lambda i, s: (i, s[0])),
                pl.BlockSpec((toks, dim), lambda i, s: (s[0], 0)),
                pl.BlockSpec((1, 1, toks), lambda i, s: (s[0], 0, 0)),
                pl.BlockSpec((1, 1, toks), lambda i, s: (s[0], 0, 0)),
            ],
            scratch_shapes=[pltpu.VMEM((8, toks), jnp.float32), pltpu.VMEM((8, toks), jnp.float32)],
        ),
        input_output_aliases={3 + k: k for k in range(len(extra))},
        compiler_params=params(1),
        cost_estimate=pl.CostEstimate(flops=2 * rows * toks * dim, bytes_accessed=4 * rows * toks, transcendentals=rows * toks),
        name="logits",
    )(idx, hid, tab, *extra)


def place_kernel(idx_ref, act_ref, *refs):
    refs[-1][...] = act_ref[...].astype(jnp.bfloat16)


def place_call(idx, act, buf, n_chunk):
    toks, dim = act.shape
    extra = [buf] if buf is not None else []
    return pl.pallas_call(
        place_kernel,
        out_shape=jax.ShapeDtypeStruct((n_chunk * toks, dim), jnp.bfloat16),
        grid_spec=pltpu.PrefetchScalarGridSpec(
            num_scalar_prefetch=1,
            grid=(2,),
            in_specs=[pl.BlockSpec((toks // 2, dim), lambda i, s: (i, 0))] + [pl.BlockSpec(memory_space=pl.ANY)] * len(extra),
            out_specs=pl.BlockSpec((toks // 2, dim), lambda i, s: (2 * s[0] + i, 0)),
        ),
        input_output_aliases={2: 0} if extra else {},
        compiler_params=params(1),
        cost_estimate=pl.CostEstimate(flops=1000 * toks * dim, bytes_accessed=6 * toks * dim, transcendentals=0),
        name="place",
    )(idx, act, *extra)


def head_kernel(base_ref, log_ref, hid_ref, max_ref, coef_ref, lab_ref, out_ref, *, tok_count):
    tile, chunk = pl.program_id(0), pl.program_id(1)
    rows, toks = log_ref.shape
    first_row = base_ref[0] + tile * rows
    lab = lab_ref[chunk] - first_row
    row_iota = lax.broadcasted_iota(jnp.int32, (rows, toks), 0)
    scaled = jnp.exp(log_ref[...] - max_ref[chunk]) * coef_ref[chunk]
    dlog = (scaled - jnp.where(row_iota == lab, 1.0 / tok_count, 0.0)).astype(jnp.bfloat16)
    part = jnp.dot(dlog, hid_ref[pl.ds(pl.multiple_of(chunk * toks, toks), toks), :], preferred_element_type=jnp.float32)

    @pl.when(chunk == 0)
    def _():
        out_ref[...] = part

    @pl.when(chunk > 0)
    def _():
        out_ref[...] += part


def head_call(base, logits, hid, gmax, coef, labels, first_tile, n_tile, tok_count):
    n_chunk, _, toks = gmax.shape
    dim = hid.shape[1]
    full = lambda shape: pl.BlockSpec(shape, lambda i, k, s: (0,) * len(shape), pipeline_mode=pl.Buffered(1))
    return pl.pallas_call(
        functools.partial(head_kernel, tok_count=tok_count),
        out_shape=jax.ShapeDtypeStruct((n_tile * ROW_TILE, dim), jnp.float32),
        grid_spec=pltpu.PrefetchScalarGridSpec(
            num_scalar_prefetch=1,
            grid=(n_tile, n_chunk),
            in_specs=[
                pl.BlockSpec((ROW_TILE, toks), lambda i, k, s: (first_tile + i, k)),
                full(hid.shape), full(gmax.shape), full(coef.shape), full(labels.shape),
            ],
            out_specs=pl.BlockSpec((ROW_TILE, dim), lambda i, k, s: (i, 0)),
        ),
        compiler_params=params(2),
        cost_estimate=pl.CostEstimate(flops=2 * n_tile * ROW_TILE * n_chunk * toks * dim, bytes_accessed=4 * n_tile * ROW_TILE * n_chunk * toks, transcendentals=0),
        name="head_grad",
    )(base, logits, hid, gmax, coef, labels)


def lookup_kernel(base_ref, lo_ref, hi_ref, grad_ref, ids_ref, act_ref, out_ref, sq_ref, buf, sem, sq_scr):
    tile = pl.program_id(0)
    rows, _ = grad_ref.shape
    first_row = base_ref[0] + tile * rows
    out_ref[...] = grad_ref[...]
    for repl in range(2):
        first = lo_ref[repl, tile] // LOOK_CHUNK
        last = (hi_ref[repl, tile] + LOOK_CHUNK - 1) // LOOK_CHUNK

        def fetch(chunk):
            start = pl.multiple_of(chunk * LOOK_CHUNK, LOOK_CHUNK)
            return pltpu.make_async_copy(act_ref.at[repl, pl.ds(start, LOOK_CHUNK), :], buf, sem)

        def body(chunk, carry):
            copy = fetch(chunk)
            copy.start()
            ids = ids_ref[repl, chunk] - first_row
            hit = lax.broadcasted_iota(jnp.int32, (rows, LOOK_CHUNK), 0) == ids
            copy.wait()
            out_ref[...] += jnp.dot(hit.astype(jnp.bfloat16), buf[...], preferred_element_type=jnp.float32)
            return carry

        lax.fori_loop(first, jnp.where(hi_ref[repl, tile] > lo_ref[repl, tile], last, first), body, 0)

    grad = out_ref[...]
    part = jnp.sum((grad * grad).reshape(rows // 8, 8, grad.shape[1]), axis=0)

    @pl.when(tile == 0)
    def _():
        sq_scr[...] = part

    @pl.when(tile > 0)
    def _():
        sq_scr[...] += part

    @pl.when(tile == pl.num_programs(0) - 1)
    def _():
        sq_ref[...] = sq_scr[...]


def lookup_call(base, low, high, grad, ids, acts):
    rows, dim = grad.shape
    return pl.pallas_call(
        lookup_kernel,
        out_shape=[jax.ShapeDtypeStruct((rows, dim), jnp.float32), jax.ShapeDtypeStruct((8, dim), jnp.float32)],
        grid_spec=pltpu.PrefetchScalarGridSpec(
            num_scalar_prefetch=3,
            grid=(rows // LOOK_TILE,),
            in_specs=[
                pl.BlockSpec((LOOK_TILE, dim), lambda i, *s: (i, 0)),
                pl.BlockSpec(ids.shape, lambda i, *s: (0, 0, 0, 0)),
                pl.BlockSpec(memory_space=pl.ANY),
            ],
            out_specs=[pl.BlockSpec((LOOK_TILE, dim), lambda i, *s: (i, 0)), pl.BlockSpec((8, dim), lambda i, *s: (0, 0))],
            scratch_shapes=[pltpu.VMEM((LOOK_CHUNK, dim), jnp.bfloat16), pltpu.SemaphoreType.DMA, pltpu.VMEM((8, dim), jnp.float32)],
        ),
        input_output_aliases={3: 0},
        compiler_params=params(1),
        cost_estimate=pl.CostEstimate(flops=4 * rows * 1024 * dim, bytes_accessed=8 * rows * dim, transcendentals=0),
        name="lookup",
    )(base, low, high, grad, ids, acts)


def adamw_kernel(pos_ref, scale_ref, grad_ref, tab_ref, avg_ref, sq_ref, *refs):
    out_tab, out_avg, out_sq, out_bf = refs[-4:]
    grad = grad_ref[...] * scale_ref[0]
    new_avg = BETA_ONE * avg_ref[...] + (1.0 - BETA_ONE) * grad
    new_sq = BETA_TWO * sq_ref[...] + (1.0 - BETA_TWO) * grad * grad
    step_dir = (new_avg * (1.0 / (1.0 - BETA_ONE ** OPT_STEP))) / (jnp.sqrt(new_sq * (1.0 / (1.0 - BETA_TWO ** OPT_STEP))) + ADAM_EPS)
    master = tab_ref[...]
    new_tab = master - LEARN_RATE * (step_dir + WEIGHT_DECAY * master)
    out_tab[...] = new_tab
    out_avg[...] = new_avg
    out_sq[...] = new_sq
    out_bf[...] = new_tab.astype(jnp.bfloat16)


def adamw_call(pos, scale, grad, grad_tile, n_tile, state, bufs):
    rows, dim = state[0].shape
    extra = list(bufs) if bufs is not None else []
    here = pl.BlockSpec((ADAM_TILE, dim), lambda i, p: (p[0] + i, 0))
    return pl.pallas_call(
        adamw_kernel,
        out_shape=[jax.ShapeDtypeStruct((rows, dim), jnp.float32)] * 3 + [jax.ShapeDtypeStruct((rows, dim), jnp.bfloat16)],
        grid_spec=pltpu.PrefetchScalarGridSpec(
            num_scalar_prefetch=1,
            grid=(n_tile,),
            in_specs=[
                pl.BlockSpec(memory_space=pltpu.SMEM),
                pl.BlockSpec((ADAM_TILE, dim), lambda i, p: (grad_tile + i, 0)),
                here, here, here,
            ] + [pl.BlockSpec(memory_space=pl.ANY)] * len(extra),
            out_specs=[here] * 4,
        ),
        input_output_aliases={6 + k: k for k in range(len(extra))},
        compiler_params=params(1),
        cost_estimate=pl.CostEstimate(flops=200 * n_tile * ADAM_TILE * dim, bytes_accessed=30 * n_tile * ADAM_TILE * dim, transcendentals=0),
        name="adamw",
    )(pos, scale, grad, *state, *extra)


def solution(mesh):
    n_stage = mesh.shape["pp"]
    n_repl = mesh.shape["dp"]
    table_spec = P("tp", None)
    last = n_stage - 1

    def spread(chunks, source, hold):
        pp_idx = lax.axis_index("pp")
        is_src = pp_idx == source
        n_chunk = len(chunks)
        n_private = n_chunk // 3
        n_direct = n_chunk - n_private
        own, other = [None] * n_chunk, [None] * n_chunk
        relay = [None] * n_direct
        for j in range(n_direct):
            relay[j] = lax.ppermute(chunks[j], "pp", [(source, hold)])
            own[j] = jnp.where(is_src, chunks[j], relay[j])
            near = lax.ppermute(chunks[j], ("dp", "pp"), [(source, n_stage + source), (n_stage + source, source)])
            far = lax.ppermute(relay[j], ("dp", "pp"), [(hold, n_stage + hold), (n_stage + hold, hold)])
            other[j] = jnp.where(is_src, near, far)
            if j < n_private:
                got = lax.ppermute(relay[j], ("tp", "pp"), [(hold, n_stage + hold), (n_stage + hold, hold)])
                own[n_chunk - 1 - j] = jnp.where(is_src, chunks[n_chunk - 1 - j], got)
                other[n_chunk - 1 - j] = lax.ppermute(
                    other[j], ("tp", "pp"),
                    [(hold, n_stage + hold), (n_stage + hold, hold), (source, n_stage + source), (n_stage + source, source)])
        holder = jnp.logical_or(is_src, pp_idx == hold)
        to_core = [(source, source ^ 1), (hold, hold ^ 1)]
        share = lambda v: jnp.where(holder, v, lax.ppermute(v, "pp", to_core))
        return [share(v) for v in own], [share(v) for v in other]

    def device_step(master, exp_avg, exp_avg_sq, stage_ids, stage_acts):
        vocab_dev, dim = master.shape
        n_seq, seq_len = stage_ids.shape[1:]
        tok_count = n_seq * seq_len
        tp_idx, dp_idx, pp_idx = lax.axis_index("tp"), lax.axis_index("dp"), lax.axis_index("pp")
        rows_own = vocab_dev // n_stage
        row_first = pp_idx * rows_own
        base = (tp_idx * vocab_dev + row_first).astype(jnp.int32)

        ids_all = lax.all_gather(stage_ids.reshape(tok_count), ("dp", "pp"), axis=0, tiled=False).reshape(n_repl, n_stage, tok_count)
        labels = ids_all[:, last].reshape(n_repl * n_seq, 1, seq_len)
        ids_sorted, order = lax.sort_key_val(ids_all[:, 0], lax.broadcasted_iota(jnp.int32, (n_repl, tok_count), 1), dimension=1)

        seq_of = lambda j: jnp.where(tp_idx == 0, j, n_seq - 1 - j)
        acts = stage_acts[0]
        hid_chunks = [lax.dynamic_index_in_dim(acts, seq_of(j), 0, keepdims=False).astype(jnp.float32) for j in range(n_seq)]
        own, other = spread(hid_chunks, last, 1)

        tab_own = lax.dynamic_slice_in_dim(master, row_first, rows_own, 0).astype(jnp.bfloat16)
        bufs = None
        arrival = [(dp_idx, j, own[j]) for j in range(n_seq)] + [(1 - dp_idx, j, other[j]) for j in range(n_seq)]
        for repl, j, chunk in arrival:
            idx = (repl * n_seq + seq_of(j)).astype(jnp.int32).reshape(1)
            bufs = logits_call(idx, chunk, tab_own, bufs, n_repl * n_seq)
        logits, hidden, loc_max, loc_sum = bufs

        look_rows = lax.dynamic_index_in_dim(order, dp_idx, 0, keepdims=False)
        act_sorted = jnp.take(acts.reshape(tok_count, dim), look_rows, axis=0).reshape(n_seq, seq_len, dim)
        act_sorted, _ = lax.optimization_barrier((act_sorted, own[3][:8]))
        act_chunks = [lax.dynamic_index_in_dim(act_sorted, seq_of(j), 0, keepdims=False).astype(jnp.float32) for j in range(n_seq)]
        dx_own, dx_other = spread(act_chunks, 0, 2)
        dx_all = None
        for repl, j, chunk in [(dp_idx, j, dx_own[j]) for j in range(n_seq)] + [(1 - dp_idx, j, dx_other[j]) for j in range(n_seq)]:
            idx = (repl * n_seq + seq_of(j)).astype(jnp.int32).reshape(1)
            dx_all = place_call(idx, chunk, dx_all, n_repl * n_seq)
        dx_all = dx_all.reshape(n_repl, tok_count, dim)

        stats = lax.all_gather(jnp.stack([loc_max, loc_sum]), ("tp", "pp"), axis=0, tiled=False)
        gmax = jnp.max(stats[:, 0], axis=0)
        coef = 1.0 / (jnp.sum(stats[:, 1] * jnp.exp(stats[:, 0] - gmax[None]), axis=0) * tok_count)

        n_part = rows_own // ROW_TILE
        half = ROW_TILE // 2
        n_look = ROW_TILE // LOOK_TILE
        ids_blocks = ids_sorted.reshape(n_repl, tok_count // LOOK_CHUNK, 1, LOOK_CHUNK)
        edges = base + LOOK_TILE * jnp.arange(rows_own // LOOK_TILE + 1, dtype=jnp.int32)
        below = jnp.sum((ids_sorted[:, None, :] < edges[None, :, None]).astype(jnp.int32), axis=2)
        cross = [(0, 2), (2, 0), (1, 3), (3, 1)]
        parts, far_parts, squares = [], [], []
        for k in range(n_part):
            start = (base + k * ROW_TILE).reshape(1)
            grad = head_call(start, logits, hidden, gmax, coef, labels, k, 1, tok_count)
            span = slice(k * n_look, (k + 1) * n_look)
            grad, square = lookup_call(start, below[:, :-1][:, span], below[:, 1:][:, span], grad, ids_blocks, dx_all)
            parts.append(grad)
            squares.append(square)
            sent = lax.ppermute(lax.dynamic_slice_in_dim(grad, dp_idx * half, half, 0), "pp", cross)
            back = lax.ppermute(sent, "dp", [(0, 1), (1, 0)])
            far_parts.append(jnp.where(dp_idx == 0, jnp.concatenate([sent, back]), jnp.concatenate([back, sent])))

        sq_total = lax.psum(jnp.sum(sum(squares)), ("tp", "pp")) / (n_repl * n_repl)
        scale = ((CLIP_NORM / jnp.maximum(jnp.sqrt(sq_total), CLIP_NORM)) / n_repl).reshape(1)

        state = (master, exp_avg, exp_avg_sq)
        swap = [(0, 1), (1, 0), (2, 3), (3, 2)]
        per = ROW_TILE // ADAM_TILE
        out = None
        for pieces, owner in (
            (parts, pp_idx),
            ([lax.ppermute(p, "pp", swap) for p in parts], pp_idx ^ 1),
            (far_parts, pp_idx ^ 2),
            ([lax.ppermute(p, "pp", swap) for p in far_parts], pp_idx ^ 3),
        ):
            for k, piece in enumerate(pieces):
                pos = (owner * (rows_own // ADAM_TILE) + k * per).astype(jnp.int32).reshape(1)
                out = adamw_call(pos, scale, piece, 0, per, state, out)
        return tuple(out)

    return jax.shard_map(
        device_step, mesh=mesh,
        in_specs=(table_spec, table_spec, table_spec, P("pp", "dp", None), P("pp", "dp", None, None)),
        out_specs=(table_spec, table_spec, table_spec, table_spec), check_vma=False)
```

```python
import functools

import jax
import jax.numpy as jnp
from jax import lax
from jax.experimental import pallas as pl
from jax.experimental.pallas import tpu as pltpu
from jax.sharding import PartitionSpec as P

LEARN_RATE = 0.003
BETA_ONE = 0.9
BETA_TWO = 0.95
ADAM_EPS = 1e-8
WEIGHT_DECAY = 0.1
CLIP_NORM = 1.0
OPT_STEP = 10

ROW_TILE = 800
TOK_CHUNK = 1536
TOK_SLICE = 256
LOOK_CHUNK = 256
ADAM_TILE = 200
VMEM_LIMIT = 63 * 1024 * 1024
LOWEST = float(jnp.finfo(jnp.float32).min)


def params(n_axes):
    return pltpu.CompilerParams(dimension_semantics=("arbitrary",) * n_axes, vmem_limit_bytes=VMEM_LIMIT)


def logits_kernel(hid_ref, tab_ref, *refs):
    out_ref, hid_out, max_out, sum_out, max_scr, sum_scr = refs[-6:]
    step = pl.program_id(1)

    @pl.when(step == 0)
    def _():
        hid_out[...] = hid_ref[...].astype(jnp.bfloat16)
        max_scr[...] = jnp.full_like(max_scr, LOWEST)
        sum_scr[...] = jnp.zeros_like(sum_scr)

    rows, toks = out_ref.shape
    for first in range(0, toks, TOK_SLICE):
        here = pl.ds(first, TOK_SLICE)
        logits = lax.dot_general(tab_ref[...], hid_out[here, :], (((1,), (1,)), ((), ())), preferred_element_type=jnp.float32)
        out_ref[:, here] = logits
        grouped = logits.reshape(rows // 8, 8, TOK_SLICE)
        old_max = max_scr[:, here]
        new_max = jnp.maximum(old_max, jnp.max(grouped, axis=0))
        sum_scr[:, here] = sum_scr[:, here] * jnp.exp(old_max - new_max) + jnp.sum(jnp.exp(grouped - new_max[None]), axis=0)
        max_scr[:, here] = new_max

    @pl.when(step == pl.num_programs(1) - 1)
    def _():
        top = jnp.max(max_scr[...], axis=0, keepdims=True)
        max_out[...] = top[None]
        sum_out[...] = jnp.sum(sum_scr[...] * jnp.exp(max_scr[...] - top), axis=0, keepdims=True)[None]


def logits_call(hid, tab, bufs, first_chunk, n_chunk):
    rows, dim = tab.shape
    toks = TOK_CHUNK
    shapes = [
        jax.ShapeDtypeStruct((rows, n_chunk * toks), jnp.float32),
        jax.ShapeDtypeStruct((n_chunk * toks, dim), jnp.bfloat16),
        jax.ShapeDtypeStruct((n_chunk, 1, toks), jnp.float32),
        jax.ShapeDtypeStruct((n_chunk, 1, toks), jnp.float32),
    ]
    extra = list(bufs) if bufs is not None else []
    here = hid.shape[0]
    return pl.pallas_call(
        logits_kernel,
        out_shape=shapes,
        grid=(here // toks, rows // ROW_TILE),
        in_specs=[
            pl.BlockSpec((toks, dim), lambda j, i: (j, 0)),
            pl.BlockSpec((ROW_TILE, dim), lambda j, i: (i, 0)),
        ] + [pl.BlockSpec(memory_space=pl.ANY)] * len(extra),
        out_specs=[
            pl.BlockSpec((ROW_TILE, toks), lambda j, i: (i, first_chunk + j)),
            pl.BlockSpec((toks, dim), lambda j, i: (first_chunk + j, 0)),
            pl.BlockSpec((1, 1, toks), lambda j, i: (first_chunk + j, 0, 0)),
            pl.BlockSpec((1, 1, toks), lambda j, i: (first_chunk + j, 0, 0)),
        ],
        scratch_shapes=[pltpu.VMEM((8, toks), jnp.float32), pltpu.VMEM((8, toks), jnp.float32)],
        input_output_aliases={2 + k: k for k in range(len(extra))},
        compiler_params=params(2),
        cost_estimate=pl.CostEstimate(flops=2 * rows * here * dim, bytes_accessed=4 * rows * here, transcendentals=rows * here),
        name="logits",
    )(hid, tab, *extra)


def head_kernel(base_ref, log_ref, hid_ref, max_ref, coef_ref, lab_ref, out_ref, even_scr, odd_scr, *, tok_count):
    tile, step = pl.program_id(0), pl.program_id(1)
    rows = log_ref.shape[0]
    toks = log_ref.shape[1] // 2
    first_row = base_ref[0] + tile * rows
    row_iota = lax.broadcasted_iota(jnp.int32, (rows, toks), 0)

    def dlogits(part):
        chunk = 2 * step + part
        scaled = jnp.exp(log_ref[:, part * toks:(part + 1) * toks] - max_ref[chunk]) * coef_ref[chunk]
        return (scaled - jnp.where(row_iota == lab_ref[chunk] - first_row, 1.0 / tok_count, 0.0)).astype(jnp.bfloat16)

    def matmul(dlog, chunk):
        return jnp.dot(dlog, hid_ref[pl.ds(pl.multiple_of(chunk * toks, toks), toks), :], preferred_element_type=jnp.float32)

    @pl.when(step == 0)
    def _():
        out_ref[...] = jnp.zeros_like(out_ref)
        odd_scr[...] = jnp.zeros_like(odd_scr)

    even_scr[...] = dlogits(0)
    out_ref[...] += matmul(odd_scr[...], jnp.maximum(2 * step - 1, 0))
    odd_scr[...] = dlogits(1)
    out_ref[...] += matmul(even_scr[...], 2 * step)

    @pl.when(step == pl.num_programs(1) - 1)
    def _():
        out_ref[...] += matmul(odd_scr[...], 2 * step + 1)


def head_call(base, logits, hid, gmax, coef, labels, tok_count):
    n_chunk, _, toks = gmax.shape
    rows, dim = logits.shape[0], hid.shape[1]
    full = lambda shape: pl.BlockSpec(shape, lambda i, k, s: (0,) * len(shape), pipeline_mode=pl.Buffered(1))
    return pl.pallas_call(
        functools.partial(head_kernel, tok_count=tok_count),
        out_shape=jax.ShapeDtypeStruct((rows, dim), jnp.float32),
        grid_spec=pltpu.PrefetchScalarGridSpec(
            num_scalar_prefetch=1,
            grid=(rows // ROW_TILE, n_chunk // 2),
            in_specs=[
                pl.BlockSpec((ROW_TILE, 2 * toks), lambda i, k, s: (i, k)),
                full(hid.shape), full(gmax.shape), full(coef.shape), full(labels.shape),
            ],
            out_specs=pl.BlockSpec((ROW_TILE, dim), lambda i, k, s: (i, 0)),
            scratch_shapes=[pltpu.VMEM((ROW_TILE, toks), jnp.bfloat16), pltpu.VMEM((ROW_TILE, toks), jnp.bfloat16)],
        ),
        compiler_params=params(2),
        cost_estimate=pl.CostEstimate(flops=2 * rows * n_chunk * toks * dim, bytes_accessed=4 * rows * n_chunk * toks, transcendentals=0),
        name="head_grad",
    )(base, logits, hid, gmax, coef, labels)


def lookup_kernel(base_ref, half_ref, lo_ref, hi_ref, grad_ref, ids_ref, act_ref, out_ref, send_ref, sq_ref, bufs, sems, *, n_list):
    rows, dim = grad_ref.shape
    first_row = base_ref[0]

    def fetch(part, chunk):
        start = pl.multiple_of(chunk * LOOK_CHUNK, LOOK_CHUNK)
        return pltpu.make_async_copy(act_ref.at[part, pl.ds(start, LOOK_CHUNK), :], bufs.at[part], sems.at[part])

    def add(part, chunk):
        hit = lax.broadcasted_iota(jnp.int32, (rows, LOOK_CHUNK), 0) == ids_ref[part, chunk] - first_row
        out_ref[...] += jnp.dot(hit.astype(jnp.bfloat16), bufs[part].astype(jnp.bfloat16), preferred_element_type=jnp.float32)

    top = ids_ref.shape[1] - 1
    first = [jnp.minimum(lo_ref[part] // LOOK_CHUNK, top) for part in range(n_list)]
    for part in range(n_list):
        fetch(part, first[part]).start()
    out_ref[...] = grad_ref[...]
    for part in range(n_list):
        fetch(part, first[part]).wait()
        add(part, first[part])

        def body(chunk, carry):
            copy = fetch(part, chunk)
            copy.start()
            copy.wait()
            add(part, chunk)
            return carry

        lax.fori_loop(first[part] + 1, (hi_ref[part] + LOOK_CHUNK - 1) // LOOK_CHUNK, body, 0)
    grad = out_ref[...]
    sq_ref[...] = jnp.sum((grad * grad).reshape(rows // 8, 8, dim), axis=0)
    send_ref[...] = out_ref[pl.ds(pl.multiple_of(half_ref[0] * (rows // 2), rows // 2), rows // 2), :]


def lookup_call(base, half, low, high, grad, tile, ids, acts):
    dim = grad.shape[1]
    n_list = ids.shape[0]
    return pl.pallas_call(
        functools.partial(lookup_kernel, n_list=n_list),
        out_shape=[
            jax.ShapeDtypeStruct((ROW_TILE, dim), jnp.float32),
            jax.ShapeDtypeStruct((ROW_TILE // 2, dim), jnp.float32),
            jax.ShapeDtypeStruct((8, dim), jnp.float32),
        ],
        grid_spec=pltpu.PrefetchScalarGridSpec(
            num_scalar_prefetch=4,
            grid=(1,),
            in_specs=[
                pl.BlockSpec((ROW_TILE, dim), lambda i, *s: (tile, 0)),
                pl.BlockSpec(ids.shape, lambda i, *s: (0, 0, 0, 0)),
                pl.BlockSpec(memory_space=pl.ANY),
            ],
            out_specs=[
                pl.BlockSpec((ROW_TILE, dim), lambda i, *s: (0, 0)),
                pl.BlockSpec((ROW_TILE // 2, dim), lambda i, *s: (0, 0)),
                pl.BlockSpec((8, dim), lambda i, *s: (0, 0)),
            ],
            scratch_shapes=[pltpu.VMEM((n_list, LOOK_CHUNK, dim), jnp.float32), pltpu.SemaphoreType.DMA((n_list,))],
        ),
        compiler_params=params(1),
        cost_estimate=pl.CostEstimate(flops=4 * ROW_TILE * 1024 * dim, bytes_accessed=12 * ROW_TILE * dim, transcendentals=0),
        name="lookup",
    )(base, half, low, high, grad, ids, acts)


def after(value, token):
    return pl.pallas_call(
        lambda value_ref, token_ref, out_ref: None,
        out_shape=jax.ShapeDtypeStruct(value.shape, value.dtype),
        in_specs=[pl.BlockSpec(memory_space=pl.ANY)] * 2,
        out_specs=pl.BlockSpec(memory_space=pl.ANY),
        input_output_aliases={0: 0},
        name="after",
    )(value, token)


def adamw_kernel(pos_ref, scale_ref, grad_ref, tab_ref, avg_ref, sq_ref, *refs):
    out_tab, out_avg, out_sq, out_bf, token = refs[-5:]
    token[...] = jnp.zeros_like(token)
    grad = grad_ref[...] * scale_ref[0]
    new_avg = BETA_ONE * avg_ref[...] + (1.0 - BETA_ONE) * grad
    new_sq = BETA_TWO * sq_ref[...] + (1.0 - BETA_TWO) * grad * grad
    step_dir = (new_avg * (1.0 / (1.0 - BETA_ONE ** OPT_STEP))) / (jnp.sqrt(new_sq * (1.0 / (1.0 - BETA_TWO ** OPT_STEP))) + ADAM_EPS)
    master = tab_ref[...]
    new_tab = master - LEARN_RATE * (step_dir + WEIGHT_DECAY * master)
    out_tab[...] = new_tab
    out_avg[...] = new_avg
    out_sq[...] = new_sq
    out_bf[...] = new_tab.astype(jnp.bfloat16)


def adamw_call(pos, scale, grad, grad_tile, n_tile, state, bufs):
    rows, dim = state[0].shape
    extra = list(bufs) if bufs is not None else []
    here = pl.BlockSpec((ADAM_TILE, dim), lambda i, p: (p[0] + i, 0))
    return pl.pallas_call(
        adamw_kernel,
        out_shape=[jax.ShapeDtypeStruct((rows, dim), jnp.float32)] * 3
        + [jax.ShapeDtypeStruct((rows, dim), jnp.bfloat16), jax.ShapeDtypeStruct((8, 128), jnp.float32)],
        grid_spec=pltpu.PrefetchScalarGridSpec(
            num_scalar_prefetch=1,
            grid=(n_tile,),
            in_specs=[
                pl.BlockSpec(memory_space=pltpu.SMEM),
                pl.BlockSpec((ADAM_TILE, dim), lambda i, p: (grad_tile + i, 0)),
                here, here, here,
            ] + [pl.BlockSpec(memory_space=pl.ANY)] * len(extra),
            out_specs=[here] * 4 + [pl.BlockSpec((8, 128), lambda i, p: (0, 0))],
        ),
        input_output_aliases={6 + k: k for k in range(len(extra))},
        compiler_params=params(1),
        cost_estimate=pl.CostEstimate(flops=200 * n_tile * ADAM_TILE * dim, bytes_accessed=30 * n_tile * ADAM_TILE * dim, transcendentals=0),
        name="adamw",
    )(pos, scale, grad, *state, *extra)


def solution(mesh):
    n_stage = mesh.shape["pp"]
    n_repl = mesh.shape["dp"]
    n_block = mesh.shape["tp"]
    table_spec = P("tp", None)
    last = n_stage - 1
    everyone = ("tp", "dp", "pp")

    def scatter(piece_of, source):
        pieces = [piece_of(p).astype(jnp.float32) for p in range(n_stage)]
        mine = jnp.where(lax.axis_index("pp") == source, pieces[source], 0.0)
        for p in range(n_stage):
            if p != source:
                mine = mine + lax.ppermute(pieces[p], "pp", [(source, p)])
        return mine

    def device_step(master, exp_avg, exp_avg_sq, stage_ids, stage_acts):
        vocab_dev, dim = master.shape
        n_seq, seq_len = stage_ids.shape[1:]
        tok_count = n_seq * seq_len
        tok_all = n_repl * tok_count
        piece = tok_count // (n_block * n_stage)
        half_piece = piece // 2
        tp_idx, dp_idx, pp_idx = lax.axis_index("tp"), lax.axis_index("dp"), lax.axis_index("pp")
        rows_own = vocab_dev // n_stage
        row_first = pp_idx * rows_own
        base = (tp_idx * vocab_dev + row_first).astype(jnp.int32)
        acts = stage_acts[0].reshape(tok_count, dim)

        def hid_piece(first):
            return lambda p: lax.dynamic_slice_in_dim(acts, (tp_idx * n_stage + p) * piece + first, half_piece, 0)

        halves = [scatter(hid_piece(h * half_piece), last) for h in range(2)]
        gathered = [lax.all_gather(v, everyone, axis=0, tiled=True) for v in halves]

        tab_own = lax.dynamic_slice_in_dim(master, row_first, rows_own, 0).astype(jnp.bfloat16)
        n_chunk = tok_all // TOK_CHUNK
        bufs = None
        for h in range(2):
            bufs = logits_call(gathered[h], tab_own, bufs, h * n_chunk // 2, n_chunk)
        logits, hidden, loc_max, loc_sum = bufs

        ids_all = lax.all_gather(stage_ids.reshape(tok_count), ("dp", "pp"), axis=0, tiled=False).reshape(n_repl, n_stage, tok_count)
        labels = ids_all[:, last].reshape(n_repl, n_block, n_stage, 2, half_piece).transpose(3, 1, 0, 2, 4).reshape(2 * n_chunk, 1, TOK_CHUNK // 2)
        ids_sorted, order = lax.sort_key_val(ids_all[:, 0], lax.broadcasted_iota(jnp.int32, (n_repl, tok_count), 1), dimension=1)
        look_rows = lax.dynamic_index_in_dim(order, dp_idx, 0, keepdims=False)
        act_sorted = acts.at[look_rows].get(mode="promise_in_bounds")
        mine = scatter(lambda p: lax.dynamic_slice_in_dim(act_sorted, (tp_idx * n_stage + p) * piece, piece, 0), 0)
        dx_all = lax.all_gather(mine, everyone, axis=0, tiled=True).reshape(n_block * n_repl, tok_count // n_block, dim)
        ids_lists = ids_sorted.reshape(n_repl, n_block, tok_count // n_block).transpose(1, 0, 2).reshape(n_block * n_repl, tok_count // n_block)
        ids_blocks = ids_lists.reshape(n_block * n_repl, -1, 1, LOOK_CHUNK)

        stats = lax.all_gather(jnp.stack([loc_max, loc_sum]), ("tp", "pp"), axis=0, tiled=False)
        gmax = jnp.max(stats[:, 0], axis=0)
        coef = 1.0 / (jnp.sum(stats[:, 1] * jnp.exp(stats[:, 0] - gmax[None]), axis=0) * tok_count)
        per_chunk = lambda v: v.reshape(2 * n_chunk, 1, TOK_CHUNK // 2)
        grad_all = head_call(base.reshape(1), logits, hidden, per_chunk(gmax), per_chunk(coef), labels, tok_count)

        n_part = rows_own // ROW_TILE
        half = ROW_TILE // 2
        edges = base + ROW_TILE * jnp.arange(n_part + 1, dtype=jnp.int32)
        below = jnp.sum((ids_lists[None] < edges[:, None, None]).astype(jnp.int32), axis=2)
        cross = [(0, 2), (2, 0), (1, 3), (3, 1)]
        swap = [(0, 1), (1, 0), (2, 3), (3, 2)]
        parts, sent, squares = [], [], []
        for k in range(n_part):
            part, send, square = lookup_call(
                (base + k * ROW_TILE).reshape(1), dp_idx.astype(jnp.int32).reshape(1), below[k], below[k + 1], grad_all, k, ids_blocks, dx_all)
            parts.append(part)
            squares.append(square)
            sent.append(lax.ppermute(send, "pp", cross))
        near = [lax.ppermute(p, "pp", swap) for p in parts]

        sq_total = lax.psum(jnp.sum(sum(squares)), ("tp", "pp")) / (n_repl * n_repl)
        scale = ((CLIP_NORM / jnp.maximum(jnp.sqrt(sq_total), CLIP_NORM)) / n_repl).reshape(1)
        state = (master, exp_avg, exp_avg_sq)
        out, token = None, None

        def update(piece, owner, k, second):
            nonlocal out, token
            tiles = piece.shape[0] // ADAM_TILE
            pos = owner * (rows_own // ADAM_TILE) + k * (ROW_TILE // ADAM_TILE)
            if second is not None:
                pos = pos + second * tiles
            *out, token = adamw_call(pos.astype(jnp.int32).reshape(1), scale, piece, 0, tiles, state, out)

        back, sent_near, back_near = {}, {}, {}

        def forward(k):
            sent[k] = after(sent[k], token)
            back[k] = lax.ppermute(sent[k], "dp", [(0, 1), (1, 0)])

        def share(k):
            sent_near[k] = lax.ppermute(sent[k], "pp", swap)

        def share_back(k):
            back[k] = after(back[k], token)
            back_near[k] = lax.ppermute(back[k], "pp", swap)

        def far(k):
            update(sent[k], pp_idx ^ 2, k, dp_idx)
            update(back[k], pp_idx ^ 2, k, 1 - dp_idx)

        def far_near(k):
            update(sent_near[k], pp_idx ^ 3, k, dp_idx)
            update(back_near[k], pp_idx ^ 3, k, 1 - dp_idx)

        for k in range(3):
            update(parts[k], pp_idx, k, None)
        forward(0)
        for k in range(3, n_part):
            update(parts[k], pp_idx, k, None)
        for k in range(2):
            update(near[k], pp_idx ^ 1, k, None)
        forward(1)
        share(0)
        for k in range(2, n_part):
            update(near[k], pp_idx ^ 1, k, None)
        forward(2)
        for k in range(n_part):
            share_back(k)
            if k >= 1:
                far_near(k - 1)
            if k + 1 < n_part:
                share(k + 1)
            far(k)
            if k + 3 < n_part:
                forward(k + 3)
        far_near(n_part - 1)
        return tuple(out)

    return jax.shard_map(
        device_step, mesh=mesh,
        in_specs=(table_spec, table_spec, table_spec, P("pp", "dp", None), P("pp", "dp", None, None)),
        out_specs=(table_spec, table_spec, table_spec, table_spec), check_vma=False)
```

```python
import functools

import jax
import jax.numpy as jnp
from jax import lax
from jax.experimental import pallas as pl
from jax.experimental.pallas import tpu as pltpu
from jax.sharding import PartitionSpec as P


LEARN_RATE = 0.003
BETA_ONE = 0.9
BETA_TWO = 0.95
ADAM_EPS = 1e-8
WEIGHT_DECAY = 0.1
CLIP_NORM = 1.0
OPT_STEP = 10

ROW_TILE = 800
TOK_CHUNK = 1536
TOK_SLICE = 256
LOOK_CHUNK = 256
ADAM_TILE = 200
VMEM_LIMIT = 63 * 1024 * 1024
LOWEST = float(jnp.finfo(jnp.float32).min)


def params(n_axes):
    return pltpu.CompilerParams(dimension_semantics=("arbitrary",) * n_axes, vmem_limit_bytes=VMEM_LIMIT)


def logits_kernel(hid_ref, tab_ref, *refs):
    out_ref, hid_out, max_out, sum_out, token, max_scr, sum_scr = refs[-7:]
    step = pl.program_id(1)
    token[...] = jnp.zeros_like(token)

    @pl.when(step == 0)
    def _():
        hid_out[...] = hid_ref[...].astype(jnp.bfloat16)
        max_scr[...] = jnp.full_like(max_scr, LOWEST)
        sum_scr[...] = jnp.zeros_like(sum_scr)

    rows, toks = out_ref.shape
    for first in range(0, toks, TOK_SLICE):
        here = pl.ds(first, TOK_SLICE)
        logits = lax.dot_general(tab_ref[...], hid_out[here, :], (((1,), (1,)), ((), ())), preferred_element_type=jnp.float32)
        out_ref[:, here] = logits
        grouped = logits.reshape(rows // 8, 8, TOK_SLICE)
        old_max = max_scr[:, here]
        new_max = jnp.maximum(old_max, jnp.max(grouped, axis=0))
        sum_scr[:, here] = sum_scr[:, here] * jnp.exp(old_max - new_max) + jnp.sum(jnp.exp(grouped - new_max[None]), axis=0)
        max_scr[:, here] = new_max

    @pl.when(step == pl.num_programs(1) - 1)
    def _():
        top = jnp.max(max_scr[...], axis=0, keepdims=True)
        max_out[...] = top[None]
        sum_out[...] = jnp.sum(sum_scr[...] * jnp.exp(max_scr[...] - top), axis=0, keepdims=True)[None]


def logits_call(hid, tab, bufs, first_chunk, n_chunk):
    rows, dim = tab.shape
    toks = TOK_CHUNK
    shapes = [
        jax.ShapeDtypeStruct((rows, n_chunk * toks), jnp.float32),
        jax.ShapeDtypeStruct((n_chunk * toks, dim), jnp.bfloat16),
        jax.ShapeDtypeStruct((n_chunk, 1, toks), jnp.float32),
        jax.ShapeDtypeStruct((n_chunk, 1, toks), jnp.float32),
        jax.ShapeDtypeStruct((8, 128), jnp.float32),
    ]
    extra = list(bufs) if bufs is not None else []
    here = hid.shape[0]
    return pl.pallas_call(
        logits_kernel,
        out_shape=shapes,
        grid=(here // toks, rows // ROW_TILE),
        in_specs=[
            pl.BlockSpec((toks, dim), lambda j, i: (j, 0)),
            pl.BlockSpec((ROW_TILE, dim), lambda j, i: (i, 0)),
        ] + [pl.BlockSpec(memory_space=pl.ANY)] * len(extra),
        out_specs=[
            pl.BlockSpec((ROW_TILE, toks), lambda j, i: (i, first_chunk + j)),
            pl.BlockSpec((toks, dim), lambda j, i: (first_chunk + j, 0)),
            pl.BlockSpec((1, 1, toks), lambda j, i: (first_chunk + j, 0, 0)),
            pl.BlockSpec((1, 1, toks), lambda j, i: (first_chunk + j, 0, 0)),
            pl.BlockSpec((8, 128), lambda j, i: (0, 0)),
        ],
        scratch_shapes=[pltpu.VMEM((8, toks), jnp.float32), pltpu.VMEM((8, toks), jnp.float32)],
        input_output_aliases={2 + k: k for k in range(len(extra))},
        compiler_params=params(2),
        cost_estimate=pl.CostEstimate(flops=2 * rows * here * dim, bytes_accessed=4 * rows * here, transcendentals=rows * here),
        name="logits",
    )(hid, tab, *extra)


def head_kernel(base_ref, log_ref, hid_ref, max_ref, coef_ref, lab_ref, out_ref, even_scr, odd_scr, *, tok_count):
    tile, step = pl.program_id(0), pl.program_id(1)
    rows = log_ref.shape[0]
    toks = log_ref.shape[1] // 2
    first_row = base_ref[0] + tile * rows
    row_iota = lax.broadcasted_iota(jnp.int32, (rows, toks), 0)

    def dlogits(part):
        chunk = 2 * step + part
        scaled = jnp.exp(log_ref[:, part * toks:(part + 1) * toks] - max_ref[chunk]) * coef_ref[chunk]
        return (scaled - jnp.where(row_iota == lab_ref[chunk] - first_row, 1.0 / tok_count, 0.0)).astype(jnp.bfloat16)

    def matmul(dlog, chunk):
        return jnp.dot(dlog, hid_ref[pl.ds(pl.multiple_of(chunk * toks, toks), toks), :], preferred_element_type=jnp.float32)

    @pl.when(step == 0)
    def _():
        out_ref[...] = jnp.zeros_like(out_ref)
        odd_scr[...] = jnp.zeros_like(odd_scr)

    even_scr[...] = dlogits(0)
    out_ref[...] += matmul(odd_scr[...], jnp.maximum(2 * step - 1, 0))
    odd_scr[...] = dlogits(1)
    out_ref[...] += matmul(even_scr[...], 2 * step)

    @pl.when(step == pl.num_programs(1) - 1)
    def _():
        out_ref[...] += matmul(odd_scr[...], 2 * step + 1)


def head_call(base, logits, hid, gmax, coef, labels, first_tile, n_tile, tok_count):
    n_chunk, _, toks = gmax.shape
    rows, dim = n_tile * ROW_TILE, hid.shape[1]
    full = lambda shape: pl.BlockSpec(shape, lambda i, k, s: (0,) * len(shape), pipeline_mode=pl.Buffered(1))
    return pl.pallas_call(
        functools.partial(head_kernel, tok_count=tok_count),
        out_shape=jax.ShapeDtypeStruct((rows, dim), jnp.float32),
        grid_spec=pltpu.PrefetchScalarGridSpec(
            num_scalar_prefetch=1,
            grid=(n_tile, n_chunk // 2),
            in_specs=[
                pl.BlockSpec((ROW_TILE, 2 * toks), lambda i, k, s: (first_tile + i, k)),
                full(hid.shape), full(gmax.shape), full(coef.shape), full(labels.shape),
            ],
            out_specs=pl.BlockSpec((ROW_TILE, dim), lambda i, k, s: (i, 0)),
            scratch_shapes=[pltpu.VMEM((ROW_TILE, toks), jnp.bfloat16), pltpu.VMEM((ROW_TILE, toks), jnp.bfloat16)],
        ),
        compiler_params=params(2),
        cost_estimate=pl.CostEstimate(flops=2 * rows * n_chunk * toks * dim, bytes_accessed=4 * rows * n_chunk * toks, transcendentals=0),
        name="head_grad",
    )(base, logits, hid, gmax, coef, labels)


def lookup_kernel(base_ref, half_ref, lo_ref, hi_ref, grad_ref, ids_ref, act_ref, out_ref, sq_ref, *refs, n_list):
    *send_refs, bufs, sems = refs
    tile = pl.program_id(0)
    rows, dim = grad_ref.shape
    first_row = base_ref[0] + tile * rows

    def fetch(part, chunk, slot):
        start = pl.multiple_of(chunk * LOOK_CHUNK, LOOK_CHUNK)
        return pltpu.make_async_copy(act_ref.at[part, pl.ds(start, LOOK_CHUNK), :], bufs.at[part, slot], sems.at[part, slot])

    top = ids_ref.shape[1] - 1
    first = [jnp.minimum(lo_ref[tile, part] // LOOK_CHUNK, top) for part in range(n_list)]
    for part in range(n_list):
        fetch(part, first[part], 0).start()
    out_ref[...] = grad_ref[...]
    for part in range(n_list):
        end = jnp.maximum((hi_ref[tile, part] + LOOK_CHUNK - 1) // LOOK_CHUNK, first[part] + 1)

        def body(chunk, carry):
            slot = lax.rem(chunk - first[part], 2)

            @pl.when(chunk + 1 < end)
            def _():
                fetch(part, chunk + 1, 1 - slot).start()

            hit = lax.broadcasted_iota(jnp.int32, (rows, LOOK_CHUNK), 0) == ids_ref[part, chunk] - first_row
            fetch(part, chunk, slot).wait()
            out_ref[...] += jnp.dot(hit.astype(jnp.bfloat16), bufs[part, slot].astype(jnp.bfloat16), preferred_element_type=jnp.float32)
            return carry

        lax.fori_loop(first[part], end, body, 0)
    grad = out_ref[...]
    square = jnp.sum((grad * grad).reshape(rows // 8, 8, dim), axis=0)

    @pl.when(tile == 0)
    def _():
        sq_ref[...] = square

    @pl.when(tile > 0)
    def _():
        sq_ref[...] += square

    for k, send_ref in enumerate(send_refs):
        @pl.when(tile == k)
        def _():
            send_ref[...] = out_ref[pl.ds(pl.multiple_of(half_ref[0] * (rows // 2), rows // 2), rows // 2), :]


def lookup_call(base, half, low, high, grad, ids, acts):
    rows, dim = grad.shape
    n_list = ids.shape[0]
    return pl.pallas_call(
        functools.partial(lookup_kernel, n_list=n_list),
        out_shape=[
            jax.ShapeDtypeStruct((rows, dim), jnp.float32),
            jax.ShapeDtypeStruct((8, dim), jnp.float32),
        ] + [jax.ShapeDtypeStruct((ROW_TILE // 2, dim), jnp.float32)] * (rows // ROW_TILE),
        grid_spec=pltpu.PrefetchScalarGridSpec(
            num_scalar_prefetch=4,
            grid=(rows // ROW_TILE,),
            in_specs=[
                pl.BlockSpec((ROW_TILE, dim), lambda i, *s: (i, 0)),
                pl.BlockSpec(ids.shape, lambda i, *s: (0, 0, 0, 0)),
                pl.BlockSpec(memory_space=pl.ANY),
            ],
            out_specs=[
                pl.BlockSpec((ROW_TILE, dim), lambda i, *s: (i, 0)),
                pl.BlockSpec((8, dim), lambda i, *s: (0, 0)),
            ] + [pl.BlockSpec((ROW_TILE // 2, dim), lambda i, *s: (0, 0))] * (rows // ROW_TILE),
            scratch_shapes=[pltpu.VMEM((n_list, 2, LOOK_CHUNK, dim), jnp.float32), pltpu.SemaphoreType.DMA((n_list, 2))],
        ),
        compiler_params=params(1),
        cost_estimate=pl.CostEstimate(flops=4 * rows * 1024 * dim, bytes_accessed=12 * rows * dim, transcendentals=0),
        name="lookup",
    )(base, half, low, high, grad, ids, acts)


def after(value, token):
    return pl.pallas_call(
        lambda value_ref, token_ref, out_ref: None,
        out_shape=jax.ShapeDtypeStruct(value.shape, value.dtype),
        in_specs=[pl.BlockSpec(memory_space=pl.ANY)] * 2,
        out_specs=pl.BlockSpec(memory_space=pl.ANY),
        input_output_aliases={0: 0},
        name="after",
    )(value, token)


def adamw_kernel(pos_ref, scale_ref, grad_ref, tab_ref, avg_ref, sq_ref, *refs):
    out_tab, out_avg, out_sq, out_bf, token = refs[-5:]
    token[...] = jnp.zeros_like(token)
    grad = grad_ref[...] * scale_ref[0]
    new_avg = BETA_ONE * avg_ref[...] + (1.0 - BETA_ONE) * grad
    new_sq = BETA_TWO * sq_ref[...] + (1.0 - BETA_TWO) * grad * grad
    step_dir = (new_avg * (1.0 / (1.0 - BETA_ONE ** OPT_STEP))) / (jnp.sqrt(new_sq * (1.0 / (1.0 - BETA_TWO ** OPT_STEP))) + ADAM_EPS)
    master = tab_ref[...]
    new_tab = master - LEARN_RATE * (step_dir + WEIGHT_DECAY * master)
    out_tab[...] = new_tab
    out_avg[...] = new_avg
    out_sq[...] = new_sq
    out_bf[...] = new_tab.astype(jnp.bfloat16)


def adamw_call(pos, scale, grad, grad_tile, n_tile, state, bufs):
    rows, dim = state[0].shape
    extra = list(bufs) if bufs is not None else []
    here = pl.BlockSpec((ADAM_TILE, dim), lambda i, p: (p[0] + i, 0))
    return pl.pallas_call(
        adamw_kernel,
        out_shape=[jax.ShapeDtypeStruct((rows, dim), jnp.float32)] * 3
        + [jax.ShapeDtypeStruct((rows, dim), jnp.bfloat16), jax.ShapeDtypeStruct((8, 128), jnp.float32)],
        grid_spec=pltpu.PrefetchScalarGridSpec(
            num_scalar_prefetch=1,
            grid=(n_tile,),
            in_specs=[
                pl.BlockSpec(memory_space=pltpu.SMEM),
                pl.BlockSpec((ADAM_TILE, dim), lambda i, p: (grad_tile + i, 0)),
                here, here, here,
            ] + [pl.BlockSpec(memory_space=pl.ANY)] * len(extra),
            out_specs=[here] * 4 + [pl.BlockSpec((8, 128), lambda i, p: (0, 0))],
        ),
        input_output_aliases={6 + k: k for k in range(len(extra))},
        compiler_params=params(1),
        cost_estimate=pl.CostEstimate(flops=200 * n_tile * ADAM_TILE * dim, bytes_accessed=30 * n_tile * ADAM_TILE * dim, transcendentals=0),
        name="adamw",
    )(pos, scale, grad, *state, *extra)


def solution(mesh):
    n_stage = mesh.shape["pp"]
    n_repl = mesh.shape["dp"]
    n_block = mesh.shape["tp"]
    table_spec = P("tp", None)
    last = n_stage - 1
    everyone = ("tp", "dp", "pp")

    def scatter(piece_of, source, token):
        pieces = [piece_of(p).astype(jnp.float32) for p in range(n_stage)]
        got = [lax.ppermute(pieces[p], "pp", [(source, p)]) for p in range(n_stage) if p != source]
        if token is not None:
            got[0] = after(got[0], token)
        return jnp.where(lax.axis_index("pp") == source, pieces[source], sum(got))

    def device_step(master, exp_avg, exp_avg_sq, stage_ids, stage_acts):
        vocab_dev, dim = master.shape
        n_seq, seq_len = stage_ids.shape[1:]
        tok_count = n_seq * seq_len
        tok_all = n_repl * tok_count
        piece = tok_count // (n_block * n_stage)
        half_piece = piece // 2
        tp_idx, dp_idx, pp_idx = lax.axis_index("tp"), lax.axis_index("dp"), lax.axis_index("pp")
        rows_own = vocab_dev // n_stage
        row_first = pp_idx * rows_own
        base = (tp_idx * vocab_dev + row_first).astype(jnp.int32)
        acts = stage_acts[0].reshape(tok_count, dim)

        def hid_piece(first):
            return lambda p: lax.dynamic_slice_in_dim(acts, (tp_idx * n_stage + p) * piece + first, half_piece, 0)

        halves = [scatter(hid_piece(0), last, None)]
        halves.append(scatter(hid_piece(half_piece), last, halves[0][:8, :128]))
        gathered = [lax.all_gather(v, everyone, axis=0, tiled=True) for v in halves]

        tab_own = lax.dynamic_slice_in_dim(master, row_first, rows_own, 0).astype(jnp.bfloat16)
        n_chunk = tok_all // TOK_CHUNK
        *bufs, first_done = logits_call(gathered[0], tab_own, None, 0, n_chunk)
        logits, hidden, loc_max, loc_sum, _ = logits_call(gathered[1], tab_own, bufs, n_chunk // 2, n_chunk)

        ids_all = lax.all_gather(stage_ids.reshape(tok_count), ("dp", "pp"), axis=0, tiled=False).reshape(n_repl, n_stage, tok_count)
        labels = ids_all[:, last].reshape(n_repl, n_block, n_stage, 2, half_piece).transpose(3, 1, 0, 2, 4).reshape(2 * n_chunk, 1, TOK_CHUNK // 2)
        ids_sorted, order = lax.sort_key_val(ids_all[:, 0], lax.broadcasted_iota(jnp.int32, (n_repl, tok_count), 1), dimension=1)
        look_rows = lax.dynamic_index_in_dim(order, dp_idx, 0, keepdims=False)
        act_sorted = acts.at[look_rows].get(mode="promise_in_bounds")
        mine = scatter(lambda p: lax.dynamic_slice_in_dim(act_sorted, (tp_idx * n_stage + p) * piece, piece, 0), 0, first_done)
        dx_all = lax.all_gather(mine, everyone, axis=0, tiled=True).reshape(n_block * n_repl, tok_count // n_block, dim)
        ids_lists = ids_sorted.reshape(n_repl, n_block, tok_count // n_block).transpose(1, 0, 2).reshape(n_block * n_repl, tok_count // n_block)
        ids_blocks = ids_lists.reshape(n_block * n_repl, -1, 1, LOOK_CHUNK)

        stats = lax.all_gather(jnp.stack([loc_max, loc_sum]), ("tp", "pp"), axis=0, tiled=False)
        gmax = jnp.max(stats[:, 0], axis=0)
        coef = 1.0 / (jnp.sum(stats[:, 1] * jnp.exp(stats[:, 0] - gmax[None]), axis=0) * tok_count)
        per_chunk = lambda v: v.reshape(2 * n_chunk, 1, TOK_CHUNK // 2)
        n_part = rows_own // ROW_TILE
        edges = base + ROW_TILE * jnp.arange(n_part + 1, dtype=jnp.int32)
        below = jnp.sum((ids_lists[None] < edges[:, None, None]).astype(jnp.int32), axis=2)
        cross = [(0, 2), (2, 0), (1, 3), (3, 1)]
        swap = [(0, 1), (1, 0), (2, 3), (3, 2)]
        groups = [(0, 3), (3, n_part - 3)]
        side = dp_idx.astype(jnp.int32).reshape(1)
        parts, sent, squares = [], [], []
        for first, count in groups:
            start = (base + first * ROW_TILE).reshape(1)
            grad = head_call(start, logits, hidden, per_chunk(gmax), per_chunk(coef), labels, first, count, tok_count)
            part, square, *send = lookup_call(start, side, below[first:first + count], below[first + 1:first + count + 1], grad, ids_blocks, dx_all)
            parts.append(part)
            squares.append(square)
            for v in send:
                sent.append(lax.ppermute(v, "pp", cross))
        near = [lax.ppermute(p, "pp", swap) for p in parts]

        sq_total = lax.psum(jnp.sum(sum(squares)), ("tp", "pp")) / (n_repl * n_repl)
        scale = ((CLIP_NORM / jnp.maximum(jnp.sqrt(sq_total), CLIP_NORM)) / n_repl).reshape(1)
        state = (master, exp_avg, exp_avg_sq)
        out, token = None, squares[1]

        def update(piece, owner, k, second):
            nonlocal out, token
            tiles = piece.shape[0] // ADAM_TILE
            pos = owner * (rows_own // ADAM_TILE) + k * (ROW_TILE // ADAM_TILE)
            if second is not None:
                pos = pos + second * tiles
            *out, token = adamw_call(pos.astype(jnp.int32).reshape(1), scale, piece, 0, tiles, state, out)

        back, sent_near, back_near = {}, {}, {}

        def forward(k):
            sent[k] = after(sent[k], token)
            back[k] = lax.ppermute(sent[k], "dp", [(0, 1), (1, 0)])

        def share(k):
            sent_near[k] = lax.ppermute(sent[k], "pp", swap)

        def share_back(k):
            back[k] = after(back[k], token)
            back_near[k] = lax.ppermute(back[k], "pp", swap)

        def far(k):
            update(sent[k], pp_idx ^ 2, k, dp_idx)
            update(back[k], pp_idx ^ 2, k, 1 - dp_idx)

        def far_near(k):
            update(sent_near[k], pp_idx ^ 3, k, dp_idx)
            update(back_near[k], pp_idx ^ 3, k, 1 - dp_idx)

        forward(0)
        forward(1)
        update(parts[0], pp_idx, groups[0][0], None)
        update(parts[1], pp_idx, groups[1][0], None)
        forward(2)
        update(near[0], pp_idx ^ 1, groups[0][0], None)
        share(0)
        update(near[1], pp_idx ^ 1, groups[1][0], None)
        share_back(0)
        forward(3)
        for k in range(n_part):
            if k >= 1:
                far_near(k - 1)
            if k + 1 < n_part:
                share(k + 1)
            if k == 1:
                forward(4)
            far(k)
            if k + 1 < n_part:
                share_back(k + 1)
        far_near(n_part - 1)
        return tuple(out)

    return jax.shard_map(
        device_step, mesh=mesh,
        in_specs=(table_spec, table_spec, table_spec, P("pp", "dp", None), P("pp", "dp", None, None)),
        out_specs=(table_spec, table_spec, table_spec, table_spec), check_vma=False)
```
